128 devices in a mesh: dp: 16 (over z, y), ep: 8 (over x, core).
Axes of the slice: x: 4, y: 4, z: 4, core: 2. Of those that a mesh axis runs over, the one named last changes fastest.
Arguments:
- x: bfloat16 [98304, 768], P(('dp', 'ep'))
- gy: bfloat16 [98304, 768], P(('dp', 'ep'))
- idx: int32 [98304], P(('dp', 'ep'))
- w_gate: bfloat16 [768, 16], replicated
- w_up: bfloat16 [16, 768, 3072], P('ep')
- w_down: bfloat16 [16, 3072, 768], P('ep')
Outputs:
- output 1: bfloat16 [98304, 768], P(('dp', 'ep'))
- output 2: bfloat16 [98304, 768], P(('dp', 'ep'))
- output 3: float32 [16, 768, 3072], P('ep')
- output 4: float32 [16, 3072, 768], P('ep')
- output 5: float32 [768, 16], replicated
All inputs are finite; a program needn't handle non-finite values.
Results may differ from the reference program's by a relative error of at most 0.00584019.
Values are sent between devices in bfloat16 or wider.
A program may use at most 1 GiB of HBM per device.

```python
import functools
import jax
import jax.numpy as jnp
from jax import lax

D_MODEL = 768
D_FF = 3072
N_EXPERTS = 16
TOKENS_DEV = 768
N_DEVICES = 128
TILE_ROWS = 128
N_TOKENS = N_DEVICES * TOKENS_DEV
CAP_ROWS = 4 * TOKENS_DEV // N_EXPERTS
N_TILES = N_TOKENS // TILE_ROWS + N_EXPERTS


def count_profile():
    hot_experts = max(1, N_EXPERTS // 16)
    cold_experts = N_EXPERTS - hot_experts
    rest_rows = TOKENS_DEV - hot_experts * CAP_ROWS
    base_rows = rest_rows // cold_experts
    extra_rows = rest_rows % cold_experts
    return [CAP_ROWS] * hot_experts + [base_rows + 1] * extra_rows + [base_rows] * (cold_experts - extra_rows)


def draw_routing(route_key):
    profile = count_profile()
    rank_table = jnp.array([rank_id for rank_id in range(N_EXPERTS) for copy_num in range(profile[rank_id])], jnp.int32)

    def one_device(dev_key):
        perm_key, shuffle_key = jax.random.split(dev_key)
        expert_perm = jax.random.permutation(perm_key, N_EXPERTS).astype(jnp.int32)
        return jax.random.permutation(shuffle_key, expert_perm[rank_table])

    return jax.vmap(one_device)(jax.random.split(route_key, N_DEVICES)).reshape(N_TOKENS)


def setup_inputs(seed: int = 0) -> dict:
    root_key = jax.random.key(seed)
    k_x, k_gy, k_gate, k_up, k_down, k_route = jax.random.split(root_key, 6)
    x = jax.random.normal(k_x, (N_TOKENS, D_MODEL), jnp.float32).astype(jnp.bfloat16)
    gy = jax.random.normal(k_gy, (N_TOKENS, D_MODEL), jnp.float32).astype(jnp.bfloat16)
    w_gate = (jax.random.normal(k_gate, (D_MODEL, N_EXPERTS), jnp.float32) * D_MODEL ** -0.5).astype(jnp.bfloat16)
    w_up = (jax.random.normal(k_up, (N_EXPERTS, D_MODEL, D_FF), jnp.float32) * D_MODEL ** -0.5).astype(jnp.bfloat16)
    w_down = (jax.random.normal(k_down, (N_EXPERTS, D_FF, D_MODEL), jnp.float32) * D_FF ** -0.5).astype(jnp.bfloat16)
    idx = draw_routing(k_route)
    return {'x': x, 'gy': gy, 'idx': idx, 'w_gate': w_gate, 'w_up': w_up, 'w_down': w_down}


def tile_pass(w_up, w_down, grad_carry, tile_in):
    grad_up, grad_down = grad_carry
    tok_rows, d_out, expert = tile_in
    up_mat = w_up[expert]
    down_mat = w_down[expert]
    pre_act = jnp.dot(tok_rows, up_mat, preferred_element_type=jnp.float32)
    hid_full, gelu_back = jax.vjp(jax.nn.gelu, pre_act)
    hidden = hid_full.astype(jnp.bfloat16)
    y_rows = jnp.dot(hidden, down_mat, preferred_element_type=jnp.float32).astype(jnp.bfloat16)
    d_hidden = jnp.dot(d_out, down_mat.T, preferred_element_type=jnp.float32)
    d_pre = gelu_back(d_hidden)[0].astype(jnp.bfloat16)
    grad_down = grad_down.at[expert].add(jnp.dot(hidden.T, d_out, preferred_element_type=jnp.float32))
    grad_up = grad_up.at[expert].add(jnp.dot(tok_rows.T, d_pre, preferred_element_type=jnp.float32))
    d_rows = jnp.dot(d_pre, up_mat.T, preferred_element_type=jnp.float32).astype(jnp.bfloat16)
    return (grad_up, grad_down), (y_rows, d_rows)


def reference(x, gy, idx, w_gate, w_up, w_down):
    onehot = idx[:, None] == jnp.arange(N_EXPERTS, dtype=jnp.int32)[None, :]
    router_logit = jnp.dot(x, w_gate, preferred_element_type=jnp.float32)
    router_prob = jax.nn.softmax(router_logit, axis=-1)
    gate_val = N_EXPERTS * jnp.sum(jnp.where(onehot, router_prob, 0.0), axis=1)
    expert_count = jnp.sum(onehot, axis=0, dtype=jnp.int32)
    sort_order = jnp.argsort(idx, stable=True)
    sorted_pos = jnp.argsort(sort_order)
    expert_start = jnp.cumsum(expert_count) - expert_count
    tile_count = (expert_count + TILE_ROWS - 1) // TILE_ROWS * TILE_ROWS
    tile_end = jnp.cumsum(tile_count)
    tile_start = tile_end - tile_count
    row_pos = tile_start[idx] + sorted_pos - expert_start[idx]
    tile_first = jnp.arange(N_TILES, dtype=jnp.int32) * TILE_ROWS
    tile_expert = jnp.minimum(jnp.sum(tile_end[None, :] <= tile_first[:, None], axis=1, dtype=jnp.int32), N_EXPERTS - 1)
    gy_full = gy.astype(jnp.float32)
    dy_tok = (gate_val[:, None] * gy_full).astype(jnp.bfloat16)
    rows_buf = jnp.zeros((N_TILES * TILE_ROWS, D_MODEL), x.dtype).at[row_pos].set(x)
    dy_buf = jnp.zeros((N_TILES * TILE_ROWS, D_MODEL), dy_tok.dtype).at[row_pos].set(dy_tok)
    grad_init = (jnp.zeros((N_EXPERTS, D_MODEL, D_FF), jnp.float32), jnp.zeros((N_EXPERTS, D_FF, D_MODEL), jnp.float32))
    tiles_in = (rows_buf.reshape(N_TILES, TILE_ROWS, D_MODEL), dy_buf.reshape(N_TILES, TILE_ROWS, D_MODEL), tile_expert)
    grads, tile_out = lax.scan(functools.partial(tile_pass, w_up, w_down), grad_init, tiles_in)
    grad_up, grad_down = grads
    y_tok = tile_out[0].reshape(N_TILES * TILE_ROWS, D_MODEL)[row_pos]
    dx_expert = tile_out[1].reshape(N_TILES * TILE_ROWS, D_MODEL)[row_pos]
    moe_out = (gate_val[:, None] * y_tok.astype(jnp.float32)).astype(jnp.bfloat16)
    d_gate = jnp.sum(gy_full * y_tok.astype(jnp.float32), axis=1)
    d_logit = ((d_gate * gate_val)[:, None] * (onehot.astype(jnp.float32) - router_prob)).astype(jnp.bfloat16)
    dx_router = jnp.dot(d_logit, w_gate.T, preferred_element_type=jnp.float32)
    grad_x = (dx_expert.astype(jnp.float32) + dx_router).astype(jnp.bfloat16)
    grad_gate = jnp.dot(x.T, d_logit, preferred_element_type=jnp.float32)
    return (moe_out, grad_x, grad_up, grad_down, grad_gate)
```

```python
import functools
import jax
import jax.numpy as jnp
from jax import lax
from jax.experimental import pallas as pl
from jax.experimental.pallas import tpu as pltpu
from jax.sharding import PartitionSpec as P

ROWS = 256
F_TILE = 512
PAD_FACTOR = 4
BF = jnp.bfloat16
F32 = jnp.float32
SQRT_2_OVER_PI = 0.7978845608028654
NT = (((1,), (1,)), ((), ()))
TN = (((0,), (0,)), ((), ()))
MIB = 1024 * 1024


def dot(a, b, dims=(((1,), (0,)), ((), ()))):
    return lax.dot_general(a, b, dims, preferred_element_type=F32)


def iota(shape, dim):
    return lax.broadcasted_iota(jnp.int32, shape, dim)


def route_kernel(cap, first_ref, idx_ref, own_ref, pos_ref, off_ref, slot_ref):
    n_src, tok = idx_ref.shape
    n_experts = own_ref.shape[0]
    first = first_ref[0]
    before = (iota((tok, tok), 0) < iota((tok, tok), 1)).astype(BF)
    idx = idx_ref[...]
    pos = jnp.full((n_src, tok), -1.0, F32)
    base = jnp.zeros((1, 1), F32)
    lane = iota((8, 128), 1)
    sub = iota((8, 128), 0)
    off = jnp.zeros((8, 128), F32)
    for j in range(2):
        hit = idx == first + j
        rank = dot(hit.astype(BF), before)
        count = jnp.sum(hit.astype(F32), axis=1, keepdims=True)
        start = base
        starts = []
        for s in range(n_src):
            starts.append(start)
            off = jnp.where((sub == j) & (lane == s), start, off)
            start = start + count[s:s + 1, :]
        off = jnp.where((sub == j) & (lane == n_src), start, off)
        pos = jnp.where(hit, jnp.concatenate(starts, axis=0) + rank, pos)
        tiles = jnp.maximum(jnp.floor((start - base + (ROWS - 1)) * (1.0 / ROWS)), 1.0)
        base = base + tiles * ROWS
        off = jnp.where((sub == 2) & (lane == j), base * (1.0 / ROWS), off)
    pos_ref[...] = pos.astype(jnp.int32)
    off_ref[...] = off.astype(jnp.int32)
    own = own_ref[...] == iota(own_ref.shape, 0)
    own_rank = dot(own.astype(BF), before)
    row = iota(own.shape, 0).astype(F32) * cap + own_rank
    slot_ref[...] = jnp.sum(jnp.where(own, row, 0.0), axis=0, keepdims=True).astype(jnp.int32)


def route(first, idx_all, idx_own, n_experts, cap):
    n_src, tok = idx_all.shape
    vm = pl.BlockSpec(memory_space=pltpu.VMEM)
    return pl.pallas_call(
        functools.partial(route_kernel, cap),
        in_specs=[pl.BlockSpec(memory_space=pltpu.SMEM), vm, vm],
        out_specs=[vm, vm, vm],
        out_shape=[
            jax.ShapeDtypeStruct((n_src, tok), jnp.int32),
            jax.ShapeDtypeStruct((8, 128), jnp.int32),
            jax.ShapeDtypeStruct((1, tok), jnp.int32),
        ],
        cost_estimate=pl.CostEstimate(flops=10**8, bytes_accessed=10**5, transcendentals=0),
        name="route",
    )(first, idx_all, jnp.broadcast_to(idx_own[None, :], (n_experts, tok)))


def gate_of(x, wg, expert):
    n_experts = wg.shape[1]
    logit = dot(x, wg)
    ex = jnp.exp(logit - jnp.max(logit, axis=1, keepdims=True))
    prob = ex / jnp.sum(ex, axis=1, keepdims=True)
    mine = iota(prob.shape, 1) == expert
    gate = n_experts * jnp.sum(jnp.where(mine, prob, 0.0), axis=1, keepdims=True)
    return prob, mine, gate


def grad_kernel(off_ref, pos_ref, x_all, gy_all, wg_ref, w1_ref, w2_ref, x_ref, gy_ref, h_ref, da_ref, d1_ref, d2_ref, x_acc, g_acc):
    step = pl.program_id(0)
    n_src = pos_ref.shape[0]
    tok = pos_ref.shape[1]
    d_ff = w1_ref.shape[2]
    local = jnp.where(step >= off_ref[2, 0], 1, 0)
    row0 = step * ROWS

    @pl.when((step == 0) | (step == off_ref[2, 0]))
    def _():
        def clear(f, carry):
            cols = pl.ds(pl.multiple_of(f * F_TILE, F_TILE), F_TILE)
            d1_ref[0, :, cols] = jnp.zeros((d1_ref.shape[1], F_TILE), F32)
            d2_ref[0, cols, :] = jnp.zeros((F_TILE, d2_ref.shape[2]), F32)
            return carry

        lax.fori_loop(0, d_ff // F_TILE, clear, 0)

    @pl.when(step < off_ref[2, 1])
    def _():
        x_acc[...] = jnp.zeros_like(x_acc)
        g_acc[...] = jnp.zeros_like(g_acc)
        for s in range(n_src):
            @pl.when((off_ref[local, s] < row0 + ROWS) & (off_ref[local, s + 1] > row0))
            def _():
                pick = (iota((ROWS, tok), 0) + row0 == pos_ref[s:s + 1, :]).astype(BF)
                rows = slice(s * tok, (s + 1) * tok)
                x_acc[...] += dot(pick, x_all[rows, :])
                g_acc[...] += dot(pick, gy_all[rows, :])
        x = x_acc[...].astype(BF)
        gy = g_acc[...]
        x_ref[...] = x
        gy_ref[...] = gy.astype(BF)
        _, _, gate = gate_of(x, wg_ref[...], off_ref[2, 2] + local)
        dy = (gate * gy).astype(BF)

        def f_step(f, carry):
            cols = pl.ds(pl.multiple_of(f * F_TILE, F_TILE), F_TILE)
            a = dot(x, w1_ref[0, :, cols])
            dh = dot(dy, w2_ref[0, cols, :], NT)
            a2 = a * a
            t = jnp.tanh(SQRT_2_OVER_PI * (a + 0.044715 * (a2 * a)))
            cdf = 0.5 * (1.0 + t)
            h = (a * cdf).astype(BF)
            slope = cdf + a * (0.5 * (1.0 - t * t)) * (SQRT_2_OVER_PI * (1.0 + (3 * 0.044715) * a2))
            da = (slope * dh).astype(BF)
            h_ref[:, cols] = h
            da_ref[:, cols] = da
            d2_ref[0, cols, :] += dot(h, dy, TN)
            d1_ref[0, :, cols] += dot(x, da, TN)
            return carry

        lax.fori_loop(0, d_ff // F_TILE, f_step, 0)


def rows_kernel(off_ref, x_ref, gy_ref, h_ref, da_ref, wg_ref, w1_ref, w2_ref, out_ref, dx_ref, dwg_ref):
    step = pl.program_id(0)

    @pl.when(step == 0)
    def _():
        dwg_ref[...] = jnp.zeros_like(dwg_ref)

    @pl.when(step < off_ref[2, 1])
    def _():
        local = jnp.where(step >= off_ref[2, 0], 1, 0)
        x = x_ref[...]
        gy = gy_ref[...].astype(F32)
        prob, mine, gate = gate_of(x, wg_ref[...], off_ref[2, 2] + local)
        y = dot(h_ref[...], w2_ref[0]).astype(BF).astype(F32)
        dxe = dot(da_ref[...], w1_ref[0], NT).astype(BF).astype(F32)
        out_ref[...] = (gate * y).astype(BF)
        d_gate = jnp.sum(gy * y, axis=1, keepdims=True)
        dz = ((d_gate * gate) * (jnp.where(mine, 1.0, 0.0) - prob)).astype(BF)
        dwg_ref[...] += dot(x, dz, TN)
        dx_ref[...] = (dxe + dot(dz, wg_ref[...], NT)).astype(BF)


def tile_map(i, off_ref):
    return (jnp.minimum(i, off_ref[2, 1] - 1), 0)


def expert_map(i, off_ref):
    return (jnp.where(i >= off_ref[2, 0], 1, 0), 0, 0)


def whole(i, off_ref):
    return (0, 0)


def one_buffer(shape, index_map):
    return pl.BlockSpec(shape, index_map, pipeline_mode=pl.Buffered(1))


def grad_pass(off, pos, x_all, gy_all, w_gate, w_up, w_down, cap_rows):
    d_model, d_ff = w_up.shape[1:]
    up_block, down_block = (1, d_model, d_ff), (1, d_ff, d_model)
    row_spec = pl.BlockSpec((ROWS, d_model), tile_map)
    hid_spec = pl.BlockSpec((ROWS, d_ff), tile_map)
    sds = jax.ShapeDtypeStruct
    return pl.pallas_call(
        grad_kernel,
        grid_spec=pltpu.PrefetchScalarGridSpec(
            num_scalar_prefetch=1,
            grid=(cap_rows // ROWS,),
            in_specs=[
                one_buffer(pos.shape, whole), one_buffer(x_all.shape, whole), one_buffer(gy_all.shape, whole),
                one_buffer(w_gate.shape, whole), one_buffer(up_block, expert_map), one_buffer(down_block, expert_map)],
            out_specs=[
                row_spec, row_spec, hid_spec, hid_spec,
                one_buffer(up_block, expert_map), one_buffer(down_block, expert_map)],
            scratch_shapes=[pltpu.VMEM((ROWS, d_model), F32), pltpu.VMEM((ROWS, d_model), F32)],
        ),
        out_shape=[
            sds((cap_rows, d_model), BF), sds((cap_rows, d_model), BF), sds((cap_rows, d_ff), BF), sds((cap_rows, d_ff), BF),
            sds(w_up.shape, F32), sds(w_down.shape, F32)],
        compiler_params=pltpu.CompilerParams(vmem_limit_bytes=63 * MIB),
        cost_estimate=pl.CostEstimate(flops=4 * 10**10, bytes_accessed=60 * MIB, transcendentals=0),
        name="grad_pass",
    )(off, pos, x_all, gy_all, w_gate, w_up, w_down)


def rows_pass(off, x_rows, gy_rows, h, da, w_gate, w_up, w_down):
    d_model, d_ff = w_up.shape[1:]
    cap_rows = x_rows.shape[0]
    row_spec = pl.BlockSpec((ROWS, d_model), tile_map)
    hid_spec = pl.BlockSpec((ROWS, d_ff), tile_map)
    sds = jax.ShapeDtypeStruct
    return pl.pallas_call(
        rows_kernel,
        grid_spec=pltpu.PrefetchScalarGridSpec(
            num_scalar_prefetch=1,
            grid=(cap_rows // ROWS,),
            in_specs=[
                row_spec, row_spec, hid_spec, hid_spec, one_buffer(w_gate.shape, whole),
                one_buffer((1, d_model, d_ff), expert_map), one_buffer((1, d_ff, d_model), expert_map)],
            out_specs=[row_spec, row_spec, one_buffer(w_gate.shape, whole)],
        ),
        out_shape=[sds(x_rows.shape, BF), sds(x_rows.shape, BF), sds(w_gate.shape, F32)],
        compiler_params=pltpu.CompilerParams(vmem_limit_bytes=48 * MIB),
        cost_estimate=pl.CostEstimate(flops=2 * 10**10, bytes_accessed=40 * MIB, transcendentals=0),
        name="rows_pass",
    )(off, x_rows, gy_rows, h, da, w_gate, w_up, w_down)


def local_step(x, gy, idx, w_gate, w_up, w_down):
    tok, d_model = x.shape
    n_experts = w_gate.shape[1]
    n_local = w_up.shape[0]
    ep = lax.axis_size('ep')
    me = lax.axis_index('ep')
    cap = PAD_FACTOR * tok // n_experts
    cap_rows = n_local * -(-ep * cap // ROWS) * ROWS

    x_all = lax.all_gather(x, 'ep', tiled=True)
    gy_all = lax.all_gather(gy, 'ep', tiled=True)
    idx_all = lax.all_gather(idx, 'ep', tiled=True).reshape(ep, tok)
    first = (me * n_local).astype(jnp.int32)
    pos, off, slot = route(first.reshape(1), idx_all, idx, n_experts, cap)
    off = off[:4, :16]
    off = lax.dynamic_update_slice(off, first.reshape(1, 1), (2, 2))

    x_rows, gy_rows, h, da, d1, d2 = grad_pass(off, pos, x_all, gy_all, w_gate, w_up, w_down, cap_rows)
    grad_up, grad_down = lax.psum((d1, d2), 'dp')
    out_rows, dx_rows, dwg = rows_pass(off, x_rows, gy_rows, h, da, w_gate, w_up, w_down)

    take = off[:n_local, :ep].T[:, :, None] + jnp.arange(cap, dtype=jnp.int32)[None, None, :]
    take = jnp.minimum(take.reshape(-1), cap_rows - 1)

    def back(rows):
        got = lax.all_to_all(rows[take].reshape(ep, n_local * cap, d_model), 'ep', 0, 0, tiled=True)
        return got.reshape(n_experts * cap, d_model)[slot.reshape(-1)]

    moe_out = back(out_rows)
    grad_x = back(dx_rows)
    grad_gate = lax.psum(dwg, ('dp', 'ep'))
    return moe_out, grad_x, grad_up, grad_down, grad_gate


def solution(mesh):
    tok_spec, exp_spec, rep = P(('dp', 'ep'), None), P('ep', None, None), P(None, None)
    return jax.shard_map(
        local_step, mesh=mesh,
        in_specs=(tok_spec, tok_spec, P(('dp', 'ep')), rep, exp_spec, exp_spec),
        out_specs=(tok_spec, tok_spec, exp_spec, exp_spec, rep),
        check_vma=False,
    )
```

```python
import functools
import jax
import jax.numpy as jnp
from jax import lax
from jax.experimental import pallas as pl
from jax.experimental.pallas import tpu as pltpu
from jax.sharding import PartitionSpec as P

ROWS = 512
PICK = 128
F_TILE = 1024
PAD_FACTOR = 4
BF = jnp.bfloat16
F32 = jnp.float32
SQRT_2_OVER_PI = 0.7978845608028654
NT = (((1,), (1,)), ((), ()))
TN = (((0,), (0,)), ((), ()))
MIB = 1024 * 1024


def dot(a, b, dims=(((1,), (0,)), ((), ()))):
    return lax.dot_general(a, b, dims, preferred_element_type=F32)


def iota(shape, dim):
    return lax.broadcasted_iota(jnp.int32, shape, dim)


def route_kernel(cap, first_ref, idx_ref, own_ref, pos_ref, off_ref, slot_ref):
    n_src, tok = idx_ref.shape
    n_experts = own_ref.shape[0]
    first = first_ref[0]
    before = (iota((tok, tok), 0) < iota((tok, tok), 1)).astype(BF)
    idx = idx_ref[...]
    pos = jnp.full((n_src, tok), -1.0, F32)
    base = jnp.zeros((1, 1), F32)
    lane = iota((8, 128), 1)
    sub = iota((8, 128), 0)
    off = jnp.zeros((8, 128), F32)
    for j in range(2):
        hit = idx == first + j
        rank = dot(hit.astype(BF), before)
        count = jnp.sum(hit.astype(F32), axis=1, keepdims=True)
        start = base
        starts = []
        for s in range(n_src):
            starts.append(start)
            off = jnp.where((sub == j) & (lane == s), start, off)
            start = start + count[s:s + 1, :]
        off = jnp.where((sub == j) & (lane == n_src), start, off)
        pos = jnp.where(hit, jnp.concatenate(starts, axis=0) + rank, pos)
        tiles = jnp.maximum(jnp.floor((start - base + (ROWS - 1)) * (1.0 / ROWS)), 1.0)
        base = base + tiles * ROWS
        off = jnp.where((sub == 2) & (lane == j), base * (1.0 / ROWS), off)
    pos_ref[...] = pos.astype(jnp.int32)
    off_ref[...] = off.astype(jnp.int32)
    own = own_ref[...] == iota(own_ref.shape, 0)
    own_rank = dot(own.astype(BF), before)
    row = iota(own.shape, 0).astype(F32) * cap + own_rank
    slot_ref[...] = jnp.sum(jnp.where(own, row, 0.0), axis=0, keepdims=True).astype(jnp.int32)


def route(first, idx_all, idx_own, n_experts, cap):
    n_src, tok = idx_all.shape
    vm = pl.BlockSpec(memory_space=pltpu.VMEM)
    return pl.pallas_call(
        functools.partial(route_kernel, cap),
        in_specs=[pl.BlockSpec(memory_space=pltpu.SMEM), vm, vm],
        out_specs=[vm, vm, vm],
        out_shape=[
            jax.ShapeDtypeStruct((n_src, tok), jnp.int32),
            jax.ShapeDtypeStruct((8, 128), jnp.int32),
            jax.ShapeDtypeStruct((1, tok), jnp.int32),
        ],
        cost_estimate=pl.CostEstimate(flops=10**8, bytes_accessed=10**5, transcendentals=0),
        name="route",
    )(first, idx_all, jnp.broadcast_to(idx_own[None, :], (n_experts, tok)))


def gate_of(x, wg, expert):
    n_experts = wg.shape[1]
    logit = dot(x, wg)
    ex = jnp.exp(logit - jnp.max(logit, axis=1, keepdims=True))
    prob = ex / jnp.sum(ex, axis=1, keepdims=True)
    mine = iota(prob.shape, 1) == expert
    gate = n_experts * jnp.sum(jnp.where(mine, prob, 0.0), axis=1, keepdims=True)
    return prob, mine, gate


def pick_kernel(off_ref, pos_ref, x_all, gy_all, x_ref, gy_ref, x_acc, g_acc):
    step = pl.program_id(0)
    n_src, tok = pos_ref.shape
    per = ROWS // PICK
    local = jnp.where(step >= off_ref[2, 0] * per, 1, 0)
    row0 = step * PICK

    @pl.when(step < off_ref[2, 1] * per)
    def _():
        x_acc[...] = jnp.zeros_like(x_acc)
        g_acc[...] = jnp.zeros_like(g_acc)
        for s in range(n_src):
            @pl.when((off_ref[local, s] < row0 + PICK) & (off_ref[local, s + 1] > row0))
            def _():
                pick = (iota((PICK, tok), 0) + row0 == pos_ref[s:s + 1, :]).astype(BF)
                x_acc[...] += dot(pick, x_all[s])
                g_acc[...] += dot(pick, gy_all[s])
        x_ref[...] = x_acc[...].astype(BF)
        gy_ref[...] = g_acc[...].astype(BF)


def grad_kernel(off_ref, x_ref, gy_ref, wg_ref, w1_ref, w2_ref, h_ref, da_ref, d1_out, d2_out, xt_ref, d1_acc, d2_acc, sem):
    step = pl.program_id(0)
    n_f = w1_ref.shape[2] // F_TILE
    total = off_ref[2, 1]
    split = off_ref[2, 0]
    local = jnp.where(step >= split, 1, 0)
    first = (step == 0) | (step == split)
    last = (step == split - 1) | (step == total - 1)

    def flush(f, which):
        cols = pl.ds(pl.multiple_of(f * F_TILE, F_TILE), F_TILE)
        return (
            pltpu.make_async_copy(d1_acc.at[:, cols], d1_out.at[which, :, cols], sem.at[0, f]),
            pltpu.make_async_copy(d2_acc.at[cols, :], d2_out.at[which, cols, :], sem.at[1, f]))

    def finish(f, which):
        for c in flush(f, which):
            c.wait()

    @pl.when(step < total)
    def _():
        x = x_ref[...]
        xt_ref[...] = x.T
        _, _, gate = gate_of(x, wg_ref[...], off_ref[2, 2] + local)
        dy = (gate * gy_ref[...].astype(F32)).astype(BF)

        def f_step(f, carry):
            cols = pl.ds(pl.multiple_of(f * F_TILE, F_TILE), F_TILE)
            a = dot(x, w1_ref[0, :, cols])
            dh = dot(dy, w2_ref[0, cols, :], NT)
            a2 = a * a
            t = jnp.tanh(a * (SQRT_2_OVER_PI + (SQRT_2_OVER_PI * 0.044715) * a2))
            cdf = 0.5 + 0.5 * t
            h = (a * cdf).astype(BF)
            slope = cdf + (0.5 * a) * (1.0 - t * t) * (SQRT_2_OVER_PI + (SQRT_2_OVER_PI * 3 * 0.044715) * a2)
            da = (slope * dh).astype(BF)
            h_ref[:, cols] = h
            da_ref[:, cols] = da

            @pl.when(step == split)
            def _():
                finish(f, 0)

            d2_acc[cols, :] = jnp.where(first, 0.0, d2_acc[cols, :]) + dot(h, dy, TN)
            d1_acc[:, cols] = jnp.where(first, 0.0, d1_acc[:, cols]) + dot(xt_ref[...], da)

            @pl.when(last)
            def _():
                for c in flush(f, local):
                    c.start()

            return carry

        lax.fori_loop(0, n_f, f_step, 0)

    @pl.when(step == total - 1)
    def _():
        def drain(f, carry):
            finish(f, 1)
            return carry

        lax.fori_loop(0, n_f, drain, 0)


def rows_kernel(off_ref, x_ref, gy_ref, h_ref, da_ref, wg_ref, w1_ref, w2_ref, out_ref, dx_ref, dwg_ref):
    step = pl.program_id(0)

    @pl.when(step == 0)
    def _():
        dwg_ref[...] = jnp.zeros_like(dwg_ref)

    @pl.when(step < off_ref[2, 1])
    def _():
        local = jnp.where(step >= off_ref[2, 0], 1, 0)
        x = x_ref[...]
        gy = gy_ref[...].astype(F32)
        prob, mine, gate = gate_of(x, wg_ref[...], off_ref[2, 2] + local)
        y = dot(h_ref[...], w2_ref[0]).astype(BF).astype(F32)
        dxe = dot(da_ref[...], w1_ref[0], NT).astype(BF).astype(F32)
        out_ref[...] = (gate * y).astype(BF)
        d_gate = jnp.sum(gy * y, axis=1, keepdims=True)
        dz = ((d_gate * gate) * (jnp.where(mine, 1.0, 0.0) - prob)).astype(BF)
        dwg_ref[...] += dot(x, dz, TN)
        dx_ref[...] = (dxe + dot(dz, wg_ref[...], NT)).astype(BF)


def tile_map(i, off_ref):
    return (jnp.minimum(i, off_ref[2, 1] - 1), 0)


def expert_map(i, off_ref):
    return (jnp.where(i >= off_ref[2, 0], 1, 0), 0, 0)


def whole(i, off_ref):
    return (0, 0)


def one_buffer(shape, index_map):
    return pl.BlockSpec(shape, index_map, pipeline_mode=pl.Buffered(1))


def gather_kernel(x_in, gy_in, idx_in, x_all, gy_all, idx_all, x_buf, gy_buf, send_r, send_l, send_p, recv_l, recv_r, recv_p, own_sem):
    n_x = lax.axis_size('ep') // 2
    me = lax.axis_index('ep')
    chip, core = me // 2, me % 2
    left = (chip + n_x - 1) % n_x * 2 + core
    right = (chip + 1) % n_x * 2 + core
    far = (chip + 2) % n_x * 2 + core
    partner = chip * 2 + 1 - core

    barrier = pltpu.get_barrier_semaphore()
    for peer in (left, right, partner):
        pl.semaphore_signal(barrier, inc=1, device_id={'ep': peer}, device_id_type=pl.DeviceIdType.MESH)
    pl.semaphore_wait(barrier, 3)

    half = x_in.shape[0] // 2
    top, bottom = pl.ds(0, half), pl.ds(half, half)
    pieces = [(idx_in, idx_all, None), (x_in, x_all, top), (gy_in, gy_all, top), (x_in, x_all, bottom), (gy_in, gy_all, bottom)]
    n_piece = len(pieces)
    to_right = (0, 1, 2)
    to_left = (3, 4)
    order_right = (0, 1, 3, 2, 4)
    order_left = (0, 3, 1, 4, 2)

    def at(ref, owner, rows):
        return ref.at[owner] if rows is None else ref.at[owner, rows]

    def copy(k, owner, source, send_sem, recv_sem, peer):
        src, dst, rows = pieces[k]
        if source is None:
            src = src if rows is None else src.at[rows]
        else:
            src = at(dst, source, rows)
        return pltpu.make_async_remote_copy(
            src_ref=src, dst_ref=at(dst, owner, rows), send_sem=send_sem, recv_sem=recv_sem,
            device_id={'ep': peer}, device_id_type=pl.DeviceIdType.MESH)

    right_own = [copy(k, me, None, send_r.at[k], recv_l.at[k], right) for k in range(n_piece)]
    left_own = [copy(k, me, None, send_l.at[k], recv_r.at[k], left) for k in range(n_piece)]
    part_own = [copy(k, me, None, send_p.at[k], recv_p.at[k], partner) for k in range(n_piece)]
    for a, b in zip(order_right, order_left):
        right_own[a].start()
        left_own[b].start()
    for c in part_own:
        c.start()

    own = [
        pltpu.make_async_copy(x_in, x_buf, own_sem.at[0]), pltpu.make_async_copy(gy_in, gy_buf, own_sem.at[1]),
        pltpu.make_async_copy(x_buf, x_all.at[me], own_sem.at[2]), pltpu.make_async_copy(gy_buf, gy_all.at[me], own_sem.at[3]),
        pltpu.make_async_copy(idx_in, idx_all.at[me], own_sem.at[4])]
    own[0].start()
    own[1].start()
    own[4].start()
    own[0].wait()
    own[2].start()
    own[1].wait()
    own[3].start()

    def part(k, owner, group):
        return copy(k, owner, owner, send_p.at[group * n_piece + k], recv_p.at[group * n_piece + k], partner)

    forward = {}
    part_fwd = []
    for a, b in zip(order_right, order_left):
        right_own[a].wait_recv()
        if a in to_right:
            forward[a] = copy(a, left, left, send_r.at[n_piece + a], recv_l.at[n_piece + a], right)
            forward[a].start()
        part_fwd.append(part(a, left, 1))
        part_fwd[-1].start()
        left_own[b].wait_recv()
        if b in to_left:
            forward[b] = copy(b, right, right, send_l.at[n_piece + b], recv_r.at[n_piece + b], left)
            forward[b].start()
        part_fwd.append(part(b, right, 2))
        part_fwd[-1].start()
    for k in (0, 1, 3, 2, 4):
        forward[k].wait_recv()
        part_fwd.append(part(k, far, 3))
        part_fwd[-1].start()
    for c in part_own + part_fwd:
        c.wait_recv()
    for c in right_own + left_own + part_own + part_fwd + list(forward.values()):
        c.wait_send()
    own[2].wait()
    own[3].wait()
    own[4].wait()


def gather_rows(x, gy, idx):
    n = lax.axis_size('ep')
    anywhere = pl.BlockSpec(memory_space=pl.ANY)
    sem = pltpu.SemaphoreType.DMA
    sds = jax.ShapeDtypeStruct
    return pl.pallas_call(
        gather_kernel,
        in_specs=[anywhere] * 3,
        out_specs=[anywhere] * 3,
        out_shape=[sds((n,) + x.shape, x.dtype), sds((n,) + gy.shape, gy.dtype), sds((n,) + idx.shape, idx.dtype)],
        scratch_shapes=[
            pltpu.VMEM(x.shape, x.dtype), pltpu.VMEM(gy.shape, gy.dtype),
            sem((10,)), sem((10,)), sem((20,)), sem((10,)), sem((10,)), sem((20,)), sem((5,))],
        compiler_params=pltpu.CompilerParams(collective_id=0, has_side_effects=True),
        cost_estimate=pl.CostEstimate(flops=8 * 10**10, bytes_accessed=60 * MIB, transcendentals=0),
        name="gather_rows",
    )(x, gy, idx)


def pick_pass(off, pos, x_all, gy_all, cap_rows):
    d_model = x_all.shape[2]
    per = ROWS // PICK

    def pick_map(i, off_ref):
        return (jnp.minimum(i, off_ref[2, 1] * per - 1), 0)

    def whole3(i, off_ref):
        return (0, 0, 0)

    spec = pl.BlockSpec((PICK, d_model), pick_map)
    sds = jax.ShapeDtypeStruct
    return pl.pallas_call(
        pick_kernel,
        grid_spec=pltpu.PrefetchScalarGridSpec(
            num_scalar_prefetch=1,
            grid=(cap_rows // PICK,),
            in_specs=[one_buffer(pos.shape, whole), one_buffer(x_all.shape, whole3), one_buffer(gy_all.shape, whole3)],
            out_specs=[spec, spec],
            scratch_shapes=[pltpu.VMEM((PICK, d_model), F32), pltpu.VMEM((PICK, d_model), F32)],
        ),
        out_shape=[sds((cap_rows, d_model), BF), sds((cap_rows, d_model), BF)],
        compiler_params=pltpu.CompilerParams(vmem_limit_bytes=40 * MIB),
        cost_estimate=pl.CostEstimate(flops=10**10, bytes_accessed=20 * MIB, transcendentals=0),
        name="pick_pass",
    )(off, pos, x_all, gy_all)


def grad_pass(off, x_rows, gy_rows, w_gate, w_up, w_down):
    d_model, d_ff = w_up.shape[1:]
    cap_rows = x_rows.shape[0]
    up_block, down_block = (1, d_model, d_ff), (1, d_ff, d_model)
    row_spec = pl.BlockSpec((ROWS, d_model), tile_map)
    hid_spec = pl.BlockSpec((ROWS, d_ff), tile_map)
    anywhere = pl.BlockSpec(memory_space=pl.ANY)
    sds = jax.ShapeDtypeStruct
    return pl.pallas_call(
        grad_kernel,
        grid_spec=pltpu.PrefetchScalarGridSpec(
            num_scalar_prefetch=1,
            grid=(cap_rows // ROWS,),
            in_specs=[
                row_spec, row_spec, one_buffer(w_gate.shape, whole),
                pl.BlockSpec(up_block, expert_map), pl.BlockSpec(down_block, expert_map)],
            out_specs=[hid_spec, hid_spec, anywhere, anywhere],
            scratch_shapes=[
                pltpu.VMEM((d_model, ROWS), BF), pltpu.VMEM((d_model, d_ff), F32), pltpu.VMEM((d_ff, d_model), F32),
                pltpu.SemaphoreType.DMA((2, d_ff // F_TILE))],
        ),
        out_shape=[sds((cap_rows, d_ff), BF), sds((cap_rows, d_ff), BF), sds(w_up.shape, F32), sds(w_down.shape, F32)],
        compiler_params=pltpu.CompilerParams(vmem_limit_bytes=63 * MIB),
        cost_estimate=pl.CostEstimate(flops=4 * 10**10, bytes_accessed=60 * MIB, transcendentals=0),
        name="grad_pass",
    )(off, x_rows, gy_rows, w_gate, w_up, w_down)


def rows_pass(off, x_rows, gy_rows, h, da, w_gate, w_up, w_down):
    d_model, d_ff = w_up.shape[1:]
    cap_rows = x_rows.shape[0]
    row_spec = pl.BlockSpec((ROWS, d_model), tile_map)
    hid_spec = pl.BlockSpec((ROWS, d_ff), tile_map)
    sds = jax.ShapeDtypeStruct
    return pl.pallas_call(
        rows_kernel,
        grid_spec=pltpu.PrefetchScalarGridSpec(
            num_scalar_prefetch=1,
            grid=(cap_rows // ROWS,),
            in_specs=[
                row_spec, row_spec, hid_spec, hid_spec, one_buffer(w_gate.shape, whole),
                one_buffer((1, d_model, d_ff), expert_map), one_buffer((1, d_ff, d_model), expert_map)],
            out_specs=[row_spec, row_spec, one_buffer(w_gate.shape, whole)],
        ),
        out_shape=[sds(x_rows.shape, BF), sds(x_rows.shape, BF), sds(w_gate.shape, F32)],
        compiler_params=pltpu.CompilerParams(vmem_limit_bytes=48 * MIB),
        cost_estimate=pl.CostEstimate(flops=2 * 10**10, bytes_accessed=40 * MIB, transcendentals=0),
        name="rows_pass",
    )(off, x_rows, gy_rows, h, da, w_gate, w_up, w_down)


def local_step(x, gy, idx, w_gate, w_up, w_down):
    tok, d_model = x.shape
    n_experts = w_gate.shape[1]
    n_local = w_up.shape[0]
    ep = lax.axis_size('ep')
    me = lax.axis_index('ep')
    cap = PAD_FACTOR * tok // n_experts
    cap_rows = n_local * -(-ep * cap // ROWS) * ROWS

    x_all, gy_all, idx_all = gather_rows(x, gy, idx.reshape(1, tok))
    idx_all = idx_all.reshape(ep, tok)
    first = (me * n_local).astype(jnp.int32)
    pos, off, slot = route(first.reshape(1), idx_all, idx, n_experts, cap)
    off = off[:4, :16]
    off = lax.dynamic_update_slice(off, first.reshape(1, 1), (2, 2))

    x_rows, gy_rows = pick_pass(off, pos, x_all, gy_all, cap_rows)
    h, da, d1, d2 = grad_pass(off, x_rows, gy_rows, w_gate, w_up, w_down)
    grad_up, grad_down = lax.psum((d1, d2), 'dp')
    out_rows, dx_rows, dwg = rows_pass(off, x_rows, gy_rows, h, da, w_gate, w_up, w_down)

    take = off[:n_local, :ep].T[:, :, None] + jnp.arange(cap, dtype=jnp.int32)[None, None, :]
    take = jnp.minimum(take.reshape(-1), cap_rows - 1)

    def back(rows):
        got = lax.all_to_all(rows[take].reshape(ep, n_local * cap, d_model), 'ep', 0, 0, tiled=True)
        return got.reshape(n_experts * cap, d_model)[slot.reshape(-1)]

    moe_out = back(out_rows)
    grad_x = back(dx_rows)
    grad_gate = lax.psum(dwg, ('dp', 'ep'))
    return moe_out, grad_x, grad_up, grad_down, grad_gate


def solution(mesh):
    tok_spec, exp_spec, rep = P(('dp', 'ep'), None), P('ep', None, None), P(None, None)
    return jax.shard_map(
        local_step, mesh=mesh,
        in_specs=(tok_spec, tok_spec, P(('dp', 'ep')), rep, exp_spec, exp_spec),
        out_specs=(tok_spec, tok_spec, exp_spec, exp_spec, rep),
        check_vma=False,
    )
```
